32 devices in a mesh: dp: 8 (over z, x), mp: 4 (over y, core).
Axes of the slice: x: 2, y: 2, z: 4, core: 2. Of those that a mesh axis runs over, the one named last changes fastest.
Arguments:
- gating_logits: bfloat16 [8, 3, 64, 7168], P('dp', None, None, 'mp'), may hold values from -6 to 6
- lifted_hidden_values: bfloat16 [8, 3, 64, 7168], P('dp', None, None, 'mp'), may hold values from -6 to 6
- loss_output_grad: bfloat16 [8, 3, 64, 2048], P('dp', None, None, 'mp'), may hold values from -160 to 160
- arrival_flags: int32 [8], P('dp'), may hold values from 0 to 1, as said below
- block_owner_map: int32 [8, 3], P('dp'), may hold values from 0 to 7, as said below
- decoder_multipliers: int32 [8, 3], P('dp'), may hold values from 1 to 4
- block_piece_number: int32 [8], replicated, may hold values from 1 to 2, as said below
Outputs:
- down_grad: float32 [2048, 7168], P('dp', 'mp')
The draws below stay inside these ranges and needn't reach their ends.
Inputs may be any that keep to these rules, and one draw needn't show every extreme that they name: `arrival_flags`: at least one replica survives. `block_owner_map`: row i lists the partitions (i + r + k) mod 8 for k < 3, with one r for all rows. `block_piece_number`: some partition has exactly 2 live tiles.
All inputs are finite; a program needn't handle non-finite values.
Results may differ from the reference program's by a relative error of at most 0.0042.
Values may be sent and summed in bfloat16 or wider, within the bound.
A program may use at most 128 MiB of HBM per device.

```python
import jax
import jax.numpy as jnp
from jax import lax

D = 2048
SLOTS = 3
TILE = 32
TILES = 2
TOK = 64
FF = 7168
N_DP = 8


def draw_arrival_flags(key, part):
    coin_flips = jax.random.randint(jax.random.fold_in(key, 11), (N_DP,), 0, 4)
    forced = jax.random.randint(jax.random.fold_in(key, 12), (), 0, N_DP)
    alive = jnp.where(coin_flips > 0, 1, 0)
    return jnp.where(jnp.arange(N_DP) == forced, 1, alive).astype(jnp.int32)


def draw_block_owner_map(key, part):
    rotation = jax.random.randint(jax.random.fold_in(key, 21), (), 0, N_DP)
    rows_idx = jnp.arange(N_DP, dtype=jnp.int32)[:, None]
    slot_idx = jnp.arange(SLOTS, dtype=jnp.int32)[None, :]
    return ((rows_idx + rotation + slot_idx) % N_DP).astype(jnp.int32)


def draw_block_piece_number(key, part):
    part_ids = jnp.arange(N_DP, dtype=jnp.int32)
    baseline = 1 + part_ids * (TILES - 1) // max(N_DP - 1, 1)
    jitter = jax.random.randint(jax.random.fold_in(key, 31), (N_DP,), 0, 2)
    return jnp.minimum(baseline + jitter, TILES).astype(jnp.int32)


def plant(array, own_key, low, high):
    shape = array.shape
    spot = [jax.random.randint(jax.random.fold_in(own_key, axis), (), 0, shape[axis]) for axis in range(len(shape))]
    array = array.at[tuple(spot)].set(low)
    longest = shape.index(max(shape))
    spot[longest] = (spot[longest] + 1) % shape[longest]
    return array.at[tuple(spot)].set(high)


def strengthened(entries, key, source, target, blocks, factor):
    owner, partner = [(jnp.arange(entries.shape[dim]) // (entries.shape[dim] // blocks)).reshape([-1 if axis == dim else 1 for axis in range(entries.ndim)]) for dim in (source, target)]
    chosen = jax.random.permutation(key, blocks)[partner]
    strong = (owner == chosen) | (owner == (partner + blocks // 2) % blocks)
    return jnp.where(strong, factor * entries, entries)


def shard_levels(own_key, extent, cuts, smallest, top_value):
    gain, own = 1.0, jax.random.fold_in(own_key, 6)
    for axis_at, blocks in cuts:
        steps = jnp.exp(jax.random.uniform(jax.random.fold_in(own, axis_at), (blocks,), jnp.float32, smallest / len(cuts), top_value / len(cuts)))
        gain = gain * jnp.repeat(steps, extent[axis_at] // blocks).reshape([-1 if axis == axis_at else 1 for axis in range(len(extent))])
    return gain


def normal_values(rng, dims, deviation, reach, cuts=(), held_as=jnp.bfloat16):
    result = deviation * jax.random.normal(rng, dims, jnp.float32)
    if cuts:
        result = result * shard_levels(rng, dims, cuts, -0.22, 0.18)
    return jnp.clip(result, -reach, reach).astype(held_as)


def noise_with(own_key, shape, scale, limit, cuts, heavy, held_as=jnp.bfloat16):
    result = scale * jax.random.normal(own_key, shape, jnp.float32)
    if cuts:
        result = result * shard_levels(own_key, shape, cuts, -0.22, 0.18)
    return jnp.clip(strengthened(result, jax.random.fold_in(own_key, 3), *heavy), -limit, limit).astype(held_as)


def setup_inputs(seed: int = 0) -> dict:
    key_of = jax.random.split(jax.random.key(seed), 8)
    return {
        "gating_logits": normal_values(key_of[0], (N_DP, SLOTS, TOK, FF), 1.0, 6.0, ((0, 8), (3, 4))),
        "lifted_hidden_values": normal_values(key_of[1], (N_DP, SLOTS, TOK, FF), 1.0, 6.0, ((0, 8), (3, 4))),
        "loss_output_grad": noise_with(key_of[2], (N_DP, SLOTS, TOK, D), ((N_DP * SLOTS * TOK) ** 0.5 / 2), 160.0, ((0, 8), (3, 4)), (0, 3, 8, 2.0)),
        "arrival_flags": draw_arrival_flags(jax.random.fold_in(key_of[7], 71), 0),
        "block_owner_map": draw_block_owner_map(jax.random.fold_in(key_of[7], 71), 0),
        "decoder_multipliers": plant(jax.random.randint(key_of[5], (N_DP, SLOTS), 1, 5), jax.random.fold_in(key_of[5], 1), 1, 4).astype(jnp.int32),
        "block_piece_number": draw_block_piece_number(jax.random.fold_in(key_of[7], 71), 0),
    }


def reference(gating_logits, lifted_hidden_values, loss_output_grad, arrival_flags, block_owner_map, decoder_multipliers, block_piece_number):
    part_ids = jnp.arange(N_DP, dtype=jnp.int32)
    slot_tiles = jnp.sum(jnp.where(block_owner_map[:, :, None] == part_ids[None, None, :], block_piece_number[None, None, :], 0), axis=2)
    live_rows = slot_tiles * TILE
    live_mask = jnp.arange(TOK, dtype=jnp.int32)[None, None, :] < live_rows[:, :, None]
    down_kernel_array = arrival_flags[:, None].astype(jnp.float32) * decoder_multipliers.astype(jnp.float32)
    total_tokens = jnp.sum(down_kernel_array * live_rows.astype(jnp.float32))

    def accumulate(running_total, current_inputs):
        gate_now, current_up_projection, cot_now, weight_now, live_now = current_inputs
        hidden = (jax.nn.silu(gate_now.astype(jnp.float32)) * current_up_projection.astype(jnp.float32) * live_now[:, :, None].astype(jnp.float32)).astype(jnp.bfloat16)
        scaled = hidden.astype(jnp.float32) * weight_now[:, None, None]
        contrib = jnp.einsum("ktd,ktf->df", cot_now.astype(jnp.float32), scaled, precision=lax.Precision.HIGHEST)
        return running_total + contrib, None

    start_sum = jnp.zeros((D, FF), jnp.float32)
    coded, _ = lax.scan(accumulate, start_sum, (gating_logits, lifted_hidden_values, loss_output_grad, down_kernel_array, live_mask))
    return coded / total_tokens
```

```python
import functools

import jax
import jax.numpy as jnp
from jax import lax
from jax.experimental import pallas as pl
from jax.experimental.pallas import tpu as pltpu
from jax.sharding import PartitionSpec as P

TILE = 32
CHUNK = 256


def kernel(
    sizes,
    flags_ref,
    owner_ref,
    mult_ref,
    pieces_ref,
    gate_ref,
    lift_ref,
    cot_ref,
    out_ref,
    hid,
    cot_all,
    cot_t,
    part,
    arrived,
    tok_mine,
    tok_g,
    tok_sum,
    tok_r,
    send_c,
    recv_c,
    send_h,
    recv_h,
    send_p,
    recv_p,
    send_tg,
    recv_tg,
    send_tr,
    recv_tr,
):
    G, R, M, slots, toks, chunks, rows = sizes
    d = lax.axis_index("dp")
    m = lax.axis_index("mp")
    g = d // R
    r = d % R
    own_cot = g == m

    def dev(g_to, r_to, m_to):
        return {"dp": g_to * R + r_to, "mp": m_to}

    def remote(src, dst, s, q, where):
        return pltpu.make_async_remote_copy(
            src_ref=src,
            dst_ref=dst,
            send_sem=s,
            recv_sem=q,
            device_id=where,
            device_id_type=pl.DeviceIdType.MESH,
        )

    def cot_copy(m_to):
        return remote(cot_ref, cot_all.at[g], send_c.at[m_to], recv_c.at[g], dev(m, r, m_to))

    def cot_in(g_from):
        return remote(
            cot_ref, cot_all.at[g_from], send_c.at[0], recv_c.at[g_from], dev(g_from, r, g)
        )

    def hid_copy(c, off):
        return remote(
            hid.at[c, g],
            hid.at[c, g],
            send_h.at[c, off],
            recv_h.at[c, g],
            dev((g + off) % G, r, m),
        )

    def hid_in(c, off):
        g_from = (g + off) % G
        return remote(
            hid.at[c, g_from],
            hid.at[c, g_from],
            send_h.at[c, off],
            recv_h.at[c, g_from],
            dev(g_from, r, m),
        )

    def part_copy(c, off):
        r_to = (r + off) % R
        return remote(
            part.at[c, r_to], arrived.at[c, r], send_p.at[c, off], recv_p.at[c, r], dev(g, r_to, m)
        )

    def part_in(c, off):
        r_from = (r + off) % R
        return remote(
            part.at[c, r_from],
            arrived.at[c, r_from],
            send_p.at[c, off],
            recv_p.at[c, r_from],
            dev(g, r_from, m),
        )

    def tok_copy(off):
        return remote(
            tok_mine, tok_g.at[g], send_tg.at[off], recv_tg.at[g], dev((g + off) % G, r, m)
        )

    def tok_in(off):
        g_from = (g + off) % G
        return remote(
            tok_mine, tok_g.at[g_from], send_tg.at[off], recv_tg.at[g_from], dev(g_from, r, m)
        )

    def sum_copy(off):
        return remote(
            tok_sum, tok_r.at[r], send_tr.at[off], recv_tr.at[r], dev(g, (r + off) % R, m)
        )

    def sum_in(off):
        r_from = (r + off) % R
        return remote(
            tok_sum, tok_r.at[r_from], send_tr.at[off], recv_tr.at[r_from], dev(g, r_from, m)
        )

    def over_r(body):
        def step(off, carry):
            body(off)
            return carry

        lax.fori_loop(1, R, step, 0)

    barrier = pltpu.get_barrier_semaphore()

    def greet(where):
        pl.semaphore_signal(
            barrier, inc=1, device_id=where, device_id_type=pl.DeviceIdType.MESH
        )

    for i in range(G):

        @pl.when(jnp.logical_not(jnp.logical_and(own_cot, i == g)))
        def _():
            greet(dev(i, r, g))

    for off in range(1, G):
        greet(dev((g + off) % G, r, m))
    over_r(lambda off: greet(dev(g, (r + off) % R, m)))
    pl.semaphore_wait(barrier, M + G - 1 + R - 1 - own_cot.astype(jnp.int32))

    for i in range(M):

        @pl.when(jnp.logical_not(jnp.logical_and(own_cot, i == m)))
        def _():
            cot_copy(i).start()

    @pl.when(own_cot)
    def _():
        cot_all[g] = cot_ref[...]

    flag = flags_ref[0].astype(jnp.float32)
    scales = []
    token_sum = jnp.float32(0)
    row = lax.broadcasted_iota(jnp.int32, (toks, CHUNK), 0)
    for k in range(slots):
        live = pieces_ref[owner_ref[0, k]] * TILE
        weight = flag * mult_ref[0, k].astype(jnp.float32)
        scales.append(jnp.where(row < live, weight, 0.0))
        token_sum = token_sum + weight * live.astype(jnp.float32)

    for c in range(chunks):
        cols = pl.ds(c * CHUNK, CHUNK)
        for k in range(slots):
            rk = pl.ds(k * toks, toks)
            v = gate_ref[rk, cols].astype(jnp.float32)
            u = lift_ref[rk, cols].astype(jnp.float32)
            h = v / (1.0 + jnp.exp(-v)) * u * scales[k]
            hid[c, g, rk, :] = h.astype(jnp.bfloat16)
        if c == 0:
            tok_mine[...] = jnp.full(tok_mine.shape, token_sum, jnp.float32)
        for off in range(1, G):
            hid_copy(c, off).start()
        if c == 0:
            for off in range(1, G):
                tok_copy(off).start()

    for i in range(G):

        @pl.when(jnp.logical_not(jnp.logical_and(own_cot, i == g)))
        def _():
            cot_in(i).wait_recv()

    for i in range(G):
        n = slots * toks
        cot_t[:, pl.ds(i * n, n)] = cot_all[i].T

    for c in range(chunks):
        for off in range(1, G):
            hid_in(c, off).wait_recv()
        block = hid[c].reshape(G * slots * toks, CHUNK)
        if c == 0:
            total = tok_mine[...]
            for off in range(1, G):
                tok_in(off).wait_recv()
                total = total + tok_g[(g + off) % G]
            tok_sum[...] = total

        def other(off):
            r_to = (r + off) % R
            left = cot_t[pl.ds(pl.multiple_of(r_to * rows, rows), rows), :]
            prod = jnp.dot(left, block, preferred_element_type=jnp.float32)
            part[c, r_to] = prod.astype(jnp.bfloat16)
            part_copy(c, off).start()

        over_r(other)
        if c == 0:
            over_r(lambda off: sum_copy(off).start())
        left = cot_t[pl.ds(pl.multiple_of(r * rows, rows), rows), :]
        out_ref[:, pl.ds(c * CHUNK, CHUNK)] = jnp.dot(
            left, block, preferred_element_type=jnp.float32
        )

    def add_tokens(off, total):
        sum_in(off).wait_recv()
        return total + tok_r[(r + off) % R]

    total = lax.fori_loop(1, R, add_tokens, tok_sum[...])
    inverse = (1.0 / total)[0:1, 0:1]
    for c in range(chunks):
        cols = pl.ds(c * CHUNK, CHUNK)

        def add_part(off):
            part_in(c, off).wait_recv()
            out_ref[:, cols] = out_ref[:, cols] + arrived[c, (r + off) % R].astype(jnp.float32)

        over_r(add_part)
        out_ref[:, cols] = out_ref[:, cols] * inverse

    for i in range(M):

        @pl.when(jnp.logical_not(jnp.logical_and(own_cot, i == m)))
        def _():
            cot_copy(i).wait_send()

    for off in range(1, G):
        tok_copy(off).wait_send()
        for c in range(chunks):
            hid_copy(c, off).wait_send()

    def drain(off):
        sum_copy(off).wait_send()
        for c in range(chunks):
            part_copy(c, off).wait_send()

    over_r(drain)


def on_device(
    mesh_shape,
    gating_logits,
    lifted_hidden_values,
    loss_output_grad,
    arrival_flags,
    block_owner_map,
    decoder_multipliers,
    block_piece_number,
):
    dp, M = mesh_shape
    G = M
    R = dp // G
    _, slots, toks, width = gating_logits.shape
    feats = loss_output_grad.shape[3]
    rows = feats * M // dp
    chunks = width // CHUNK
    n = slots * toks
    sizes = (G, R, M, slots, toks, chunks, rows)
    smem = pl.BlockSpec(memory_space=pltpu.SMEM)
    vmem = pl.BlockSpec(memory_space=pltpu.VMEM)
    dma = pltpu.SemaphoreType.DMA
    bf, f32 = jnp.bfloat16, jnp.float32
    return pl.pallas_call(
        functools.partial(kernel, sizes),
        out_shape=jax.ShapeDtypeStruct((rows, width), f32),
        in_specs=[smem] * 4 + [vmem] * 3,
        out_specs=vmem,
        scratch_shapes=[
            pltpu.VMEM((chunks, G, n, CHUNK), bf),
            pltpu.VMEM((G, n, feats), bf),
            pltpu.VMEM((feats, G * n), bf),
            pltpu.VMEM((chunks, R, rows, CHUNK), bf),
            pltpu.VMEM((chunks, R, rows, CHUNK), bf),
            pltpu.VMEM((8, 128), f32),
            pltpu.VMEM((G, 8, 128), f32),
            pltpu.VMEM((8, 128), f32),
            pltpu.VMEM((R, 8, 128), f32),
            dma((M,)),
            dma((G,)),
            dma((chunks, G)),
            dma((chunks, G)),
            dma((chunks, R)),
            dma((chunks, R)),
            dma((G,)),
            dma((G,)),
            dma((R,)),
            dma((R,)),
        ],
        compiler_params=pltpu.CompilerParams(
            collective_id=0, has_side_effects=True, vmem_limit_bytes=48 * 1024 * 1024
        ),
    )(
        arrival_flags,
        block_owner_map,
        decoder_multipliers,
        block_piece_number,
        gating_logits.reshape(n, width),
        lifted_hidden_values.reshape(n, width),
        loss_output_grad.reshape(n, feats),
    )


def solution(mesh):
    shape = (mesh.shape["dp"], mesh.shape["mp"])
    return jax.shard_map(
        functools.partial(on_device, shape),
        mesh=mesh,
        in_specs=(
            P("dp", None, None, "mp"),
            P("dp", None, None, "mp"),
            P("dp", None, None, "mp"),
            P("dp"),
            P("dp", None),
            P("dp", None),
            P(),
        ),
        out_specs=P("dp", "mp"),
        check_vma=False,
    )
```

```python
import functools

import jax
import jax.numpy as jnp
from jax import lax
from jax.experimental import pallas as pl
from jax.experimental.pallas import tpu as pltpu
from jax.sharding import PartitionSpec as P

TILE = 32
CHUNK = 256


def kernel(
    sizes,
    flags_ref,
    owner_ref,
    mult_ref,
    pieces_ref,
    gate_hbm,
    lift_hbm,
    cot_hbm,
    out_ref,
    gate_in,
    lift_in,
    cot_ref,
    quarters,
    hid,
    cot_all,
    cot_t,
    part,
    arrived,
    tok_mine,
    tok_g,
    tok_sum,
    tok_r,
    load_c,
    load_g,
    load_l,
    send_1,
    recv_1,
    send_2,
    recv_2,
    send_3,
    recv_3,
    send_h,
    recv_h,
    send_p,
    recv_p,
    send_tg,
    recv_tg,
    send_tr,
    recv_tr,
):
    G, R, M, slots, toks, chunks, rows = sizes
    d = lax.axis_index("dp")
    m = lax.axis_index("mp")
    g = d // R
    r = d % R
    quarter = slots * toks // M

    def dev(g_to, r_to, m_to):
        return {"dp": g_to * R + r_to, "mp": m_to}

    def remote(src, dst, s, q, where):
        return pltpu.make_async_remote_copy(
            src_ref=src,
            dst_ref=dst,
            send_sem=s,
            recv_sem=q,
            device_id=where,
            device_id_type=pl.DeviceIdType.MESH,
        )

    def spread_copy(off):
        m_to = (m + off) % M
        return remote(
            cot_ref.at[pl.ds(pl.multiple_of(m_to * quarter, quarter), quarter)],
            quarters.at[m],
            send_1.at[off],
            recv_1.at[m],
            dev(g, r, m_to),
        )

    def spread_in(off):
        m_from = (m + off) % M
        return remote(
            quarters.at[m_from],
            quarters.at[m_from],
            send_1.at[off],
            recv_1.at[m_from],
            dev(g, r, m_from),
        )

    def cross_copy(off):
        g_to = (g + off) % G
        return remote(
            quarters.at[g_to], cot_all.at[m, g], send_2.at[off], recv_2.at[g], dev(g_to, r, m)
        )

    def cross_in(off):
        g_from = (g + off) % G
        return remote(
            quarters.at[g],
            cot_all.at[m, g_from],
            send_2.at[off],
            recv_2.at[g_from],
            dev(g_from, r, m),
        )

    def share_copy(off):
        return remote(
            cot_all.at[m], cot_all.at[m], send_3.at[off], recv_3.at[m], dev(g, r, (m + off) % M)
        )

    def share_in(off):
        m_from = (m + off) % M
        return remote(
            cot_all.at[m_from],
            cot_all.at[m_from],
            send_3.at[off],
            recv_3.at[m_from],
            dev(g, r, m_from),
        )

    def load(src, dst, c, sem):
        return pltpu.make_async_copy(
            src.at[:, pl.ds(c * CHUNK, CHUNK)], dst.at[c], sem.at[c]
        )

    def hid_copy(c, off):
        return remote(
            hid.at[c, g],
            hid.at[c, g],
            send_h.at[c, off],
            recv_h.at[c, g],
            dev((g + off) % G, r, m),
        )

    def hid_in(c, off):
        g_from = (g + off) % G
        return remote(
            hid.at[c, g_from],
            hid.at[c, g_from],
            send_h.at[c, off],
            recv_h.at[c, g_from],
            dev(g_from, r, m),
        )

    def part_copy(c, off):
        r_to = (r + off) % R
        return remote(
            part.at[c, r_to], arrived.at[c, r], send_p.at[c, off], recv_p.at[c, r], dev(g, r_to, m)
        )

    def part_in(c, off):
        r_from = (r + off) % R
        return remote(
            part.at[c, r_from],
            arrived.at[c, r_from],
            send_p.at[c, off],
            recv_p.at[c, r_from],
            dev(g, r_from, m),
        )

    def tok_copy(off):
        return remote(
            tok_mine, tok_g.at[g], send_tg.at[off], recv_tg.at[g], dev((g + off) % G, r, m)
        )

    def tok_in(off):
        g_from = (g + off) % G
        return remote(
            tok_mine, tok_g.at[g_from], send_tg.at[off], recv_tg.at[g_from], dev(g_from, r, m)
        )

    def sum_copy(off):
        return remote(
            tok_sum, tok_r.at[r], send_tr.at[off], recv_tr.at[r], dev(g, (r + off) % R, m)
        )

    def sum_in(off):
        r_from = (r + off) % R
        return remote(
            tok_sum, tok_r.at[r_from], send_tr.at[off], recv_tr.at[r_from], dev(g, r_from, m)
        )

    def over_r(body):
        def step(off, carry):
            body(off)
            return carry

        lax.fori_loop(1, R, step, 0)

    load_cot = pltpu.make_async_copy(cot_hbm, cot_ref, load_c)
    load_cot.start()
    for c in range(chunks):
        load(gate_hbm, gate_in, c, load_g).start()
        load(lift_hbm, lift_in, c, load_l).start()

    barrier = pltpu.get_barrier_semaphore()

    def greet(where):
        pl.semaphore_signal(
            barrier, inc=1, device_id=where, device_id_type=pl.DeviceIdType.MESH
        )

    for off in range(1, M):
        greet(dev(g, r, (m + off) % M))
    for off in range(1, G):
        greet(dev((g + off) % G, r, m))
    over_r(lambda off: greet(dev(g, (r + off) % R, m)))
    load_cot.wait()
    quarters[m] = cot_ref[pl.ds(pl.multiple_of(m * quarter, quarter), quarter), :]
    pl.semaphore_wait(barrier, M - 1 + G - 1 + R - 1)

    for off in range(1, M):
        spread_copy(off).start()

    flag = flags_ref[0].astype(jnp.float32)
    scales = []
    token_sum = jnp.float32(0)
    row = lax.broadcasted_iota(jnp.int32, (toks, CHUNK), 0)
    for k in range(slots):
        live = pieces_ref[owner_ref[0, k]] * TILE
        weight = flag * mult_ref[0, k].astype(jnp.float32)
        scales.append(jnp.where(row < live, weight, 0.0))
        token_sum = token_sum + weight * live.astype(jnp.float32)

    for c in range(chunks):
        load(gate_hbm, gate_in, c, load_g).wait()
        load(lift_hbm, lift_in, c, load_l).wait()
        for k in range(slots):
            rk = pl.ds(k * toks, toks)
            v = gate_in[c, rk, :].astype(jnp.float32)
            u = lift_in[c, rk, :].astype(jnp.float32)
            h = v / (1.0 + jnp.exp(-v)) * u * scales[k]
            hid[c, g, rk, :] = h.astype(jnp.bfloat16)
        if c == 0:
            tok_mine[...] = jnp.full(tok_mine.shape, token_sum, jnp.float32)
        for off in range(1, G):
            hid_copy(c, off).start()
        if c == 0:
            for off in range(1, G):
                tok_copy(off).start()
            for off in range(1, M):
                spread_in(off).wait_recv()
            cot_all[m, g] = quarters[g]
            for off in range(1, G):
                cross_copy(off).start()

    for off in range(1, G):
        cross_in(off).wait_recv()
    for off in range(1, M):
        share_copy(off).start()
    for off in range(1, M):
        share_in(off).wait_recv()

    for i in range(G):
        n = slots * toks
        block = jnp.concatenate([cot_all[j, i] for j in range(M)], axis=0)
        cot_t[:, pl.ds(i * n, n)] = block.T

    for c in range(chunks):
        for off in range(1, G):
            hid_in(c, off).wait_recv()
        block = hid[c].reshape(G * slots * toks, CHUNK)
        if c == 0:
            total = tok_mine[...]
            for off in range(1, G):
                tok_in(off).wait_recv()
                total = total + tok_g[(g + off) % G]
            tok_sum[...] = total

        def other(off):
            r_to = (r + off) % R
            left = cot_t[pl.ds(pl.multiple_of(r_to * rows, rows), rows), :]
            prod = jnp.dot(left, block, preferred_element_type=jnp.float32)
            part[c, r_to] = prod.astype(jnp.bfloat16)
            part_copy(c, off).start()

        over_r(other)
        if c == 0:
            over_r(lambda off: sum_copy(off).start())
        left = cot_t[pl.ds(pl.multiple_of(r * rows, rows), rows), :]
        out_ref[:, pl.ds(c * CHUNK, CHUNK)] = jnp.dot(
            left, block, preferred_element_type=jnp.float32
        )

    def add_tokens(off, total):
        sum_in(off).wait_recv()
        return total + tok_r[(r + off) % R]

    total = lax.fori_loop(1, R, add_tokens, tok_sum[...])
    inverse = (1.0 / total)[0:1, 0:1]
    for c in range(chunks):
        cols = pl.ds(c * CHUNK, CHUNK)

        def add_part(off):
            part_in(c, off).wait_recv()
            out_ref[:, cols] = out_ref[:, cols] + arrived[c, (r + off) % R].astype(jnp.float32)

        over_r(add_part)
        out_ref[:, cols] = out_ref[:, cols] * inverse

    for off in range(1, M):
        spread_copy(off).wait_send()
        share_copy(off).wait_send()

    for off in range(1, G):
        tok_copy(off).wait_send()
        cross_copy(off).wait_send()
        for c in range(chunks):
            hid_copy(c, off).wait_send()

    def drain(off):
        sum_copy(off).wait_send()
        for c in range(chunks):
            part_copy(c, off).wait_send()

    over_r(drain)


def on_device(
    mesh_shape,
    gating_logits,
    lifted_hidden_values,
    loss_output_grad,
    arrival_flags,
    block_owner_map,
    decoder_multipliers,
    block_piece_number,
):
    dp, M = mesh_shape
    G = M
    R = dp // G
    _, slots, toks, width = gating_logits.shape
    feats = loss_output_grad.shape[3]
    rows = feats * M // dp
    chunks = width // CHUNK
    n = slots * toks
    sizes = (G, R, M, slots, toks, chunks, rows)
    smem = pl.BlockSpec(memory_space=pltpu.SMEM)
    vmem = pl.BlockSpec(memory_space=pltpu.VMEM)
    dma = pltpu.SemaphoreType.DMA
    bf, f32 = jnp.bfloat16, jnp.float32
    return pl.pallas_call(
        functools.partial(kernel, sizes),
        out_shape=jax.ShapeDtypeStruct((rows, width), f32),
        in_specs=[smem] * 4 + [pl.BlockSpec(memory_space=pl.ANY)] * 3,
        out_specs=vmem,
        scratch_shapes=[
            pltpu.VMEM((chunks, n, CHUNK), bf),
            pltpu.VMEM((chunks, n, CHUNK), bf),
            pltpu.VMEM((n, feats), bf),
            pltpu.VMEM((M, n // M, feats), bf),
            pltpu.VMEM((chunks, G, n, CHUNK), bf),
            pltpu.VMEM((M, G, n // M, feats), bf),
            pltpu.VMEM((feats, G * n), bf),
            pltpu.VMEM((chunks, R, rows, CHUNK), bf),
            pltpu.VMEM((chunks, R, rows, CHUNK), bf),
            pltpu.VMEM((8, 128), f32),
            pltpu.VMEM((G, 8, 128), f32),
            pltpu.VMEM((8, 128), f32),
            pltpu.VMEM((R, 8, 128), f32),
            dma,
            dma((chunks,)),
            dma((chunks,)),
            dma((M,)),
            dma((M,)),
            dma((G,)),
            dma((G,)),
            dma((M,)),
            dma((M,)),
            dma((chunks, G)),
            dma((chunks, G)),
            dma((chunks, R)),
            dma((chunks, R)),
            dma((G,)),
            dma((G,)),
            dma((R,)),
            dma((R,)),
        ],
        compiler_params=pltpu.CompilerParams(
            collective_id=0, has_side_effects=True
        ),
    )(
        arrival_flags,
        block_owner_map,
        decoder_multipliers,
        block_piece_number,
        gating_logits.reshape(n, width),
        lifted_hidden_values.reshape(n, width),
        loss_output_grad.reshape(n, feats),
    )


def solution(mesh):
    shape = (mesh.shape["dp"], mesh.shape["mp"])
    return jax.shard_map(
        functools.partial(on_device, shape),
        mesh=mesh,
        in_specs=(
            P("dp", None, None, "mp"),
            P("dp", None, None, "mp"),
            P("dp", None, None, "mp"),
            P("dp"),
            P("dp", None),
            P("dp", None),
            P(),
        ),
        out_specs=P("dp", "mp"),
        check_vma=False,
    )
```

```python
import functools

import jax
import jax.numpy as jnp
from jax import lax
from jax.experimental import pallas as pl
from jax.experimental.pallas import tpu as pltpu
from jax.sharding import PartitionSpec as P

TILE = 32
CHUNK = 256


def kernel(
    sizes,
    flags_ref,
    owner_ref,
    mult_ref,
    pieces_ref,
    gate_hbm,
    lift_hbm,
    cot_hbm,
    out_ref,
    gate_in,
    lift_in,
    cot_ref,
    quarters,
    hid,
    cot_all,
    cot_t,
    part,
    arrived,
    tok_mine,
    tok_g,
    tok_sum,
    tok_r,
    load_c,
    load_g,
    load_l,
    send_1,
    recv_1,
    send_2,
    recv_2,
    send_3,
    recv_3,
    send_up,
    send_dn,
    recv_h,
    send_p,
    recv_p,
    send_tg,
    recv_tg,
    send_tr,
    recv_tr,
):
    G, R, M, slots, toks, chunks, rows = sizes
    d = lax.axis_index("dp")
    m = lax.axis_index("mp")
    g = d // R
    r = d % R
    quarter = slots * toks // M

    def dev(g_to, r_to, m_to):
        return {"dp": g_to * R + r_to, "mp": m_to}

    def remote(src, dst, s, q, where):
        return pltpu.make_async_remote_copy(
            src_ref=src,
            dst_ref=dst,
            send_sem=s,
            recv_sem=q,
            device_id=where,
            device_id_type=pl.DeviceIdType.MESH,
        )

    def spread_copy(off):
        m_to = (m + off) % M
        return remote(
            cot_ref.at[pl.ds(pl.multiple_of(m_to * quarter, quarter), quarter)],
            quarters.at[m],
            send_1.at[off],
            recv_1.at[m],
            dev(g, r, m_to),
        )

    def spread_in(off):
        m_from = (m + off) % M
        return remote(
            quarters.at[m_from],
            quarters.at[m_from],
            send_1.at[off],
            recv_1.at[m_from],
            dev(g, r, m_from),
        )

    def cross_copy(off):
        g_to = (g + off) % G
        return remote(
            quarters.at[g_to], cot_all.at[m, g], send_2.at[off], recv_2.at[g], dev(g_to, r, m)
        )

    def cross_in(off):
        g_from = (g + off) % G
        return remote(
            quarters.at[g],
            cot_all.at[m, g_from],
            send_2.at[off],
            recv_2.at[g_from],
            dev(g_from, r, m),
        )

    def share_copy(off):
        return remote(
            cot_all.at[m], cot_all.at[m], send_3.at[off], recv_3.at[m], dev(g, r, (m + off) % M)
        )

    def share_in(off):
        m_from = (m + off) % M
        return remote(
            cot_all.at[m_from],
            cot_all.at[m_from],
            send_3.at[off],
            recv_3.at[m_from],
            dev(g, r, m_from),
        )

    def load(src, dst, c, sem):
        return pltpu.make_async_copy(
            src.at[:, pl.ds(c * CHUNK, CHUNK)], dst.at[c], sem.at[c]
        )

    def hop(c, origin, to, sems):
        return remote(
            hid.at[c, origin],
            hid.at[c, origin],
            sems.at[c, origin],
            recv_h.at[c, origin],
            dev(to, r, m),
        )

    up, down = (g + 1) % G, (g + G - 1) % G

    def pass_on(c, origin, has_next, to, sems):
        hop(c, origin, to, sems).wait_recv()

        @pl.when(has_next)
        def _():
            hop(c, origin, to, sems).start()

    def part_copy(c, off):
        r_to = (r + off) % R
        return remote(
            part.at[c, r_to], arrived.at[c, r], send_p.at[c, off], recv_p.at[c, r], dev(g, r_to, m)
        )

    def part_in(c, off):
        r_from = (r + off) % R
        return remote(
            part.at[c, r_from],
            arrived.at[c, r_from],
            send_p.at[c, off],
            recv_p.at[c, r_from],
            dev(g, r_from, m),
        )

    def tok_copy(off):
        return remote(
            tok_mine, tok_g.at[g], send_tg.at[off], recv_tg.at[g], dev((g + off) % G, r, m)
        )

    def tok_in(off):
        g_from = (g + off) % G
        return remote(
            tok_mine, tok_g.at[g_from], send_tg.at[off], recv_tg.at[g_from], dev(g_from, r, m)
        )

    def sum_copy(off):
        return remote(
            tok_sum, tok_r.at[r], send_tr.at[off], recv_tr.at[r], dev(g, (r + off) % R, m)
        )

    def sum_in(off):
        r_from = (r + off) % R
        return remote(
            tok_sum, tok_r.at[r_from], send_tr.at[off], recv_tr.at[r_from], dev(g, r_from, m)
        )

    def over_r(body):
        def step(off, carry):
            body(off)
            return carry

        lax.fori_loop(1, R, step, 0)

    load_cot = pltpu.make_async_copy(cot_hbm, cot_ref, load_c)
    load_cot.start()
    for c in range(chunks):
        load(gate_hbm, gate_in, c, load_g).start()
        load(lift_hbm, lift_in, c, load_l).start()

    barrier = pltpu.get_barrier_semaphore()

    def greet(where):
        pl.semaphore_signal(
            barrier, inc=1, device_id=where, device_id_type=pl.DeviceIdType.MESH
        )

    for off in range(1, M):
        greet(dev(g, r, (m + off) % M))
    for off in range(1, G):
        greet(dev((g + off) % G, r, m))
    over_r(lambda off: greet(dev(g, (r + off) % R, m)))
    load_cot.wait()
    quarters[m] = cot_ref[pl.ds(pl.multiple_of(m * quarter, quarter), quarter), :]
    pl.semaphore_wait(barrier, M - 1 + G - 1 + R - 1)

    for off in range(1, M):
        spread_copy(off).start()

    flag = flags_ref[0].astype(jnp.float32)
    scales = []
    token_sum = jnp.float32(0)
    row = lax.broadcasted_iota(jnp.int32, (toks, CHUNK), 0)
    for k in range(slots):
        live = pieces_ref[owner_ref[0, k]] * TILE
        weight = flag * mult_ref[0, k].astype(jnp.float32)
        scales.append(jnp.where(row < live, weight, 0.0))
        token_sum = token_sum + weight * live.astype(jnp.float32)

    for c in range(chunks):
        load(gate_hbm, gate_in, c, load_g).wait()
        load(lift_hbm, lift_in, c, load_l).wait()
        for k in range(slots):
            rk = pl.ds(k * toks, toks)
            v = gate_in[c, rk, :].astype(jnp.float32)
            u = lift_in[c, rk, :].astype(jnp.float32)
            h = v / (1.0 + jnp.exp(-v)) * u * scales[k]
            hid[c, g, rk, :] = h.astype(jnp.bfloat16)
        if c == 0:
            tok_mine[...] = jnp.full(tok_mine.shape, token_sum, jnp.float32)

        @pl.when(g < G - 1)
        def _():
            hop(c, g, up, send_up).start()

        @pl.when(g > 0)
        def _():
            hop(c, g, down, send_dn).start()

        if c == 0:
            for off in range(1, G):
                tok_copy(off).start()
            for off in range(1, M):
                spread_in(off).wait_recv()
            cot_all[m, g] = quarters[g]
            for off in range(1, G):
                cross_copy(off).start()

    for off in range(1, G):
        cross_in(off).wait_recv()
    for off in range(1, M):
        share_copy(off).start()
    for off in range(1, M):
        share_in(off).wait_recv()

    for i in range(G):
        n = slots * toks
        block = jnp.concatenate([cot_all[j, i] for j in range(M)], axis=0)
        cot_t[:, pl.ds(i * n, n)] = block.T

    for c in range(chunks):
        for k in range(1, G):

            @pl.when(g >= k)
            def _():
                pass_on(c, (g + G - k) % G, g < G - 1, up, send_up)

            @pl.when(g + k < G)
            def _():
                pass_on(c, (g + k) % G, g > 0, down, send_dn)

        block = hid[c].reshape(G * slots * toks, CHUNK)
        if c == 0:
            total = tok_mine[...]
            for off in range(1, G):
                tok_in(off).wait_recv()
                total = total + tok_g[(g + off) % G]
            tok_sum[...] = total

        def other(off):
            r_to = (r + off) % R
            left = cot_t[pl.ds(pl.multiple_of(r_to * rows, rows), rows), :]
            prod = jnp.dot(left, block, preferred_element_type=jnp.float32)
            part[c, r_to] = prod.astype(jnp.bfloat16)
            part_copy(c, off).start()

        over_r(other)
        if c == 0:
            over_r(lambda off: sum_copy(off).start())
        left = cot_t[pl.ds(pl.multiple_of(r * rows, rows), rows), :]
        out_ref[:, pl.ds(c * CHUNK, CHUNK)] = jnp.dot(
            left, block, preferred_element_type=jnp.float32
        )

    def add_tokens(off, total):
        sum_in(off).wait_recv()
        return total + tok_r[(r + off) % R]

    total = lax.fori_loop(1, R, add_tokens, tok_sum[...])
    inverse = (1.0 / total)[0:1, 0:1]
    for c in range(chunks):
        cols = pl.ds(c * CHUNK, CHUNK)

        def add_part(off):
            part_in(c, off).wait_recv()
            out_ref[:, cols] = out_ref[:, cols] + arrived[c, (r + off) % R].astype(jnp.float32)

        over_r(add_part)
        out_ref[:, cols] = out_ref[:, cols] * inverse

    for off in range(1, M):
        spread_copy(off).wait_send()
        share_copy(off).wait_send()

    for off in range(1, G):
        tok_copy(off).wait_send()
        cross_copy(off).wait_send()

    for c in range(chunks):
        for i in range(G):

            @pl.when(jnp.logical_and(i <= g, g < G - 1))
            def _():
                hop(c, i, up, send_up).wait_send()

            @pl.when(jnp.logical_and(i >= g, g > 0))
            def _():
                hop(c, i, down, send_dn).wait_send()

    def drain(off):
        sum_copy(off).wait_send()
        for c in range(chunks):
            part_copy(c, off).wait_send()

    over_r(drain)


def on_device(
    mesh_shape,
    gating_logits,
    lifted_hidden_values,
    loss_output_grad,
    arrival_flags,
    block_owner_map,
    decoder_multipliers,
    block_piece_number,
):
    dp, M = mesh_shape
    G = M
    R = dp // G
    _, slots, toks, width = gating_logits.shape
    feats = loss_output_grad.shape[3]
    rows = feats * M // dp
    chunks = width // CHUNK
    n = slots * toks
    sizes = (G, R, M, slots, toks, chunks, rows)
    smem = pl.BlockSpec(memory_space=pltpu.SMEM)
    vmem = pl.BlockSpec(memory_space=pltpu.VMEM)
    dma = pltpu.SemaphoreType.DMA
    bf, f32 = jnp.bfloat16, jnp.float32
    return pl.pallas_call(
        functools.partial(kernel, sizes),
        out_shape=jax.ShapeDtypeStruct((rows, width), f32),
        in_specs=[smem] * 4 + [pl.BlockSpec(memory_space=pl.ANY)] * 3,
        out_specs=vmem,
        scratch_shapes=[
            pltpu.VMEM((chunks, n, CHUNK), bf),
            pltpu.VMEM((chunks, n, CHUNK), bf),
            pltpu.VMEM((n, feats), bf),
            pltpu.VMEM((M, n // M, feats), bf),
            pltpu.VMEM((chunks, G, n, CHUNK), bf),
            pltpu.VMEM((M, G, n // M, feats), bf),
            pltpu.VMEM((feats, G * n), bf),
            pltpu.VMEM((chunks, R, rows, CHUNK), bf),
            pltpu.VMEM((chunks, R, rows, CHUNK), bf),
            pltpu.VMEM((8, 128), f32),
            pltpu.VMEM((G, 8, 128), f32),
            pltpu.VMEM((8, 128), f32),
            pltpu.VMEM((R, 8, 128), f32),
            dma,
            dma((chunks,)),
            dma((chunks,)),
            dma((M,)),
            dma((M,)),
            dma((G,)),
            dma((G,)),
            dma((M,)),
            dma((M,)),
            dma((chunks, G)),
            dma((chunks, G)),
            dma((chunks, G)),
            dma((chunks, R)),
            dma((chunks, R)),
            dma((G,)),
            dma((G,)),
            dma((R,)),
            dma((R,)),
        ],
        compiler_params=pltpu.CompilerParams(
            collective_id=0, has_side_effects=True
        ),
    )(
        arrival_flags,
        block_owner_map,
        decoder_multipliers,
        block_piece_number,
        gating_logits.reshape(n, width),
        lifted_hidden_values.reshape(n, width),
        loss_output_grad.reshape(n, feats),
    )


def solution(mesh):
    shape = (mesh.shape["dp"], mesh.shape["mp"])
    return jax.shard_map(
        functools.partial(on_device, shape),
        mesh=mesh,
        in_specs=(
            P("dp", None, None, "mp"),
            P("dp", None, None, "mp"),
            P("dp", None, None, "mp"),
            P("dp"),
            P("dp", None),
            P("dp", None),
            P(),
        ),
        out_specs=P("dp", "mp"),
        check_vma=False,
    )
```

```python
import functools

import jax
import jax.numpy as jnp
from jax import lax
from jax.experimental import pallas as pl
from jax.experimental.pallas import tpu as pltpu
from jax.sharding import PartitionSpec as P

TILE = 32
CHUNK = 256


def kernel(
    sizes,
    flags_ref,
    owner_ref,
    mult_ref,
    pieces_ref,
    gate_hbm,
    lift_hbm,
    cot_hbm,
    out_ref,
    gate_in,
    lift_in,
    cot_ref,
    quarters,
    hid,
    cot_all,
    cot_t,
    part,
    arrived,
    tok_mine,
    tok_g,
    tok_sum,
    tok_r,
    load_c,
    load_g,
    load_l,
    send_1,
    recv_1,
    send_2,
    recv_2,
    send_3,
    recv_3,
    send_up,
    send_dn,
    recv_h,
    send_p,
    recv_p,
    send_tg,
    recv_tg,
    send_tr,
    recv_tr,
):
    G, R, M, slots, toks, chunks, rows = sizes
    d = lax.axis_index("dp")
    m = lax.axis_index("mp")
    g = d // R
    r = d % R
    quarter = slots * toks // M

    def dev(g_to, r_to, m_to):
        return {"dp": g_to * R + r_to, "mp": m_to}

    def remote(src, dst, s, q, where):
        return pltpu.make_async_remote_copy(
            src_ref=src,
            dst_ref=dst,
            send_sem=s,
            recv_sem=q,
            device_id=where,
            device_id_type=pl.DeviceIdType.MESH,
        )

    def spread_copy(off):
        m_to = (m + off) % M
        return remote(
            cot_ref.at[pl.ds(pl.multiple_of(m_to * quarter, quarter), quarter)],
            quarters.at[m],
            send_1.at[off],
            recv_1.at[m],
            dev(g, r, m_to),
        )

    def spread_in(off):
        m_from = (m + off) % M
        return remote(
            quarters.at[m_from],
            quarters.at[m_from],
            send_1.at[off],
            recv_1.at[m_from],
            dev(g, r, m_from),
        )

    def cross_copy(off):
        g_to = (g + off) % G
        return remote(
            quarters.at[g_to], cot_all.at[m, g], send_2.at[off], recv_2.at[g], dev(g_to, r, m)
        )

    def cross_in(off):
        g_from = (g + off) % G
        return remote(
            quarters.at[g],
            cot_all.at[m, g_from],
            send_2.at[off],
            recv_2.at[g_from],
            dev(g_from, r, m),
        )

    def share_copy(off):
        return remote(
            cot_all.at[m], cot_all.at[m], send_3.at[off], recv_3.at[m], dev(g, r, (m + off) % M)
        )

    def share_in(off):
        m_from = (m + off) % M
        return remote(
            cot_all.at[m_from],
            cot_all.at[m_from],
            send_3.at[off],
            recv_3.at[m_from],
            dev(g, r, m_from),
        )

    def load(src, dst, c, sem):
        return pltpu.make_async_copy(
            src.at[:, pl.ds(c * CHUNK, CHUNK)], dst.at[c], sem.at[c]
        )

    def hop(c, origin, to, sems):
        return remote(
            hid.at[c, origin],
            hid.at[c, origin],
            sems.at[c, origin],
            recv_h.at[c, origin],
            dev(to, r, m),
        )

    up, down = (g + 1) % G, (g + G - 1) % G

    def pass_on(c, origin, has_next, to, sems):
        hop(c, origin, to, sems).wait_recv()

        @pl.when(has_next)
        def _():
            hop(c, origin, to, sems).start()

    def relay(c, k):
        @pl.when(g >= k)
        def _():
            pass_on(c, (g + G - k) % G, g < G - 1, up, send_up)

        @pl.when(g + k < G)
        def _():
            pass_on(c, (g + k) % G, g > 0, down, send_dn)

    def part_copy(c, off):
        r_to = (r + off) % R
        return remote(
            part.at[c, r_to], arrived.at[c, r], send_p.at[c, off], recv_p.at[c, r], dev(g, r_to, m)
        )

    def part_in(c, off):
        r_from = (r + off) % R
        return remote(
            part.at[c, r_from],
            arrived.at[c, r_from],
            send_p.at[c, off],
            recv_p.at[c, r_from],
            dev(g, r_from, m),
        )

    def tok_copy(off):
        return remote(
            tok_mine, tok_g.at[g], send_tg.at[off], recv_tg.at[g], dev((g + off) % G, r, m)
        )

    def tok_in(off):
        g_from = (g + off) % G
        return remote(
            tok_mine, tok_g.at[g_from], send_tg.at[off], recv_tg.at[g_from], dev(g_from, r, m)
        )

    def sum_copy(off):
        return remote(
            tok_sum, tok_r.at[r], send_tr.at[off], recv_tr.at[r], dev(g, (r + off) % R, m)
        )

    def sum_in(off):
        r_from = (r + off) % R
        return remote(
            tok_sum, tok_r.at[r_from], send_tr.at[off], recv_tr.at[r_from], dev(g, r_from, m)
        )

    def over_r(body):
        def step(off, carry):
            body(off)
            return carry

        lax.fori_loop(1, R, step, 0)

    load_cot = pltpu.make_async_copy(cot_hbm, cot_ref, load_c)
    load_cot.start()
    for c in range(chunks):
        load(gate_hbm, gate_in, c, load_g).start()
        load(lift_hbm, lift_in, c, load_l).start()

    barrier = pltpu.get_barrier_semaphore()

    def greet(where):
        pl.semaphore_signal(
            barrier, inc=1, device_id=where, device_id_type=pl.DeviceIdType.MESH
        )

    for off in range(1, M):
        greet(dev(g, r, (m + off) % M))
    for off in range(1, G):
        greet(dev((g + off) % G, r, m))
    over_r(lambda off: greet(dev(g, (r + off) % R, m)))
    load_cot.wait()
    quarters[m] = cot_ref[pl.ds(pl.multiple_of(m * quarter, quarter), quarter), :]
    flag = flags_ref[0].astype(jnp.float32)
    scales = []
    token_sum = jnp.float32(0)
    row = lax.broadcasted_iota(jnp.int32, (toks, CHUNK), 0)
    for k in range(slots):
        live = pieces_ref[owner_ref[0, k]] * TILE
        weight = flag * mult_ref[0, k].astype(jnp.float32)
        scales.append(jnp.where(row < live, weight, 0.0))
        token_sum = token_sum + weight * live.astype(jnp.float32)

    tok_mine[...] = jnp.full(tok_mine.shape, token_sum, jnp.float32)

    def activate(c):
        load(gate_hbm, gate_in, c, load_g).wait()
        load(lift_hbm, lift_in, c, load_l).wait()
        for k in range(slots):
            rk = pl.ds(k * toks, toks)
            v = gate_in[c, rk, :].astype(jnp.float32)
            u = lift_in[c, rk, :].astype(jnp.float32)
            h = v / (1.0 + jnp.exp(-v)) * u * scales[k]
            hid[c, g, rk, :] = h.astype(jnp.bfloat16)

    early = min(2, chunks)
    for c in range(early):
        activate(c)

    pl.semaphore_wait(barrier, M - 1 + G - 1 + R - 1)
    for off in range(1, M):
        spread_copy(off).start()

    for c in range(chunks):
        if c >= early:
            activate(c)

        @pl.when(g < G - 1)
        def _():
            hop(c, g, up, send_up).start()

        @pl.when(g > 0)
        def _():
            hop(c, g, down, send_dn).start()

        if c == 0:
            for off in range(1, G):
                tok_copy(off).start()
            for off in range(1, M):
                spread_in(off).wait_recv()
            cot_all[m, g] = quarters[g]
            for off in range(1, G):
                cross_copy(off).start()

    for off in range(1, G):
        cross_in(off).wait_recv()
    for off in range(1, M):
        share_copy(off).start()
    for c in range(chunks):
        relay(c, 1)
    for off in range(1, M):
        share_in(off).wait_recv()

    for i in range(G):
        n = slots * toks
        block = jnp.concatenate([cot_all[j, i] for j in range(M)], axis=0)
        cot_t[:, pl.ds(i * n, n)] = block.T

    for c in range(chunks):
        for k in range(2, G):
            relay(c, k)
        block = hid[c].reshape(G * slots * toks, CHUNK)
        if c == 0:
            total = tok_mine[...]
            for off in range(1, G):
                tok_in(off).wait_recv()
                total = total + tok_g[(g + off) % G]
            tok_sum[...] = total

        def other(off):
            r_to = (r + off) % R
            left = cot_t[pl.ds(pl.multiple_of(r_to * rows, rows), rows), :]
            prod = jnp.dot(left, block, preferred_element_type=jnp.float32)
            part[c, r_to] = prod.astype(jnp.bfloat16)
            part_copy(c, off).start()

        over_r(other)
        if c == 0:
            over_r(lambda off: sum_copy(off).start())
        left = cot_t[pl.ds(pl.multiple_of(r * rows, rows), rows), :]
        out_ref[:, pl.ds(c * CHUNK, CHUNK)] = jnp.dot(
            left, block, preferred_element_type=jnp.float32
        )

    def add_tokens(off, total):
        sum_in(off).wait_recv()
        return total + tok_r[(r + off) % R]

    total = lax.fori_loop(1, R, add_tokens, tok_sum[...])
    inverse = (1.0 / total)[0:1, 0:1]
    for c in range(chunks):
        cols = pl.ds(c * CHUNK, CHUNK)

        def add_part(off):
            part_in(c, off).wait_recv()
            out_ref[:, cols] = out_ref[:, cols] + arrived[c, (r + off) % R].astype(jnp.float32)

        over_r(add_part)
        out_ref[:, cols] = out_ref[:, cols] * inverse

    for off in range(1, M):
        spread_copy(off).wait_send()
        share_copy(off).wait_send()

    for off in range(1, G):
        tok_copy(off).wait_send()
        cross_copy(off).wait_send()

    for c in range(chunks):
        for i in range(G):

            @pl.when(jnp.logical_and(i <= g, g < G - 1))
            def _():
                hop(c, i, up, send_up).wait_send()

            @pl.when(jnp.logical_and(i >= g, g > 0))
            def _():
                hop(c, i, down, send_dn).wait_send()

    def drain(off):
        sum_copy(off).wait_send()
        for c in range(chunks):
            part_copy(c, off).wait_send()

    over_r(drain)


def on_device(
    mesh_shape,
    gating_logits,
    lifted_hidden_values,
    loss_output_grad,
    arrival_flags,
    block_owner_map,
    decoder_multipliers,
    block_piece_number,
):
    dp, M = mesh_shape
    G = M
    R = dp // G
    _, slots, toks, width = gating_logits.shape
    feats = loss_output_grad.shape[3]
    rows = feats * M // dp
    chunks = width // CHUNK
    n = slots * toks
    sizes = (G, R, M, slots, toks, chunks, rows)
    smem = pl.BlockSpec(memory_space=pltpu.SMEM)
    vmem = pl.BlockSpec(memory_space=pltpu.VMEM)
    dma = pltpu.SemaphoreType.DMA
    bf, f32 = jnp.bfloat16, jnp.float32
    return pl.pallas_call(
        functools.partial(kernel, sizes),
        out_shape=jax.ShapeDtypeStruct((rows, width), f32),
        in_specs=[smem] * 4 + [pl.BlockSpec(memory_space=pl.ANY)] * 3,
        out_specs=vmem,
        scratch_shapes=[
            pltpu.VMEM((chunks, n, CHUNK), bf),
            pltpu.VMEM((chunks, n, CHUNK), bf),
            pltpu.VMEM((n, feats), bf),
            pltpu.VMEM((M, n // M, feats), bf),
            pltpu.VMEM((chunks, G, n, CHUNK), bf),
            pltpu.VMEM((M, G, n // M, feats), bf),
            pltpu.VMEM((feats, G * n), bf),
            pltpu.VMEM((chunks, R, rows, CHUNK), bf),
            pltpu.VMEM((chunks, R, rows, CHUNK), bf),
            pltpu.VMEM((8, 128), f32),
            pltpu.VMEM((G, 8, 128), f32),
            pltpu.VMEM((8, 128), f32),
            pltpu.VMEM((R, 8, 128), f32),
            dma,
            dma((chunks,)),
            dma((chunks,)),
            dma((M,)),
            dma((M,)),
            dma((G,)),
            dma((G,)),
            dma((M,)),
            dma((M,)),
            dma((chunks, G)),
            dma((chunks, G)),
            dma((chunks, G)),
            dma((chunks, R)),
            dma((chunks, R)),
            dma((G,)),
            dma((G,)),
            dma((R,)),
            dma((R,)),
        ],
        compiler_params=pltpu.CompilerParams(
            collective_id=0, has_side_effects=True
        ),
    )(
        arrival_flags,
        block_owner_map,
        decoder_multipliers,
        block_piece_number,
        gating_logits.reshape(n, width),
        lifted_hidden_values.reshape(n, width),
        loss_output_grad.reshape(n, feats),
    )


def solution(mesh):
    shape = (mesh.shape["dp"], mesh.shape["mp"])
    return jax.shard_map(
        functools.partial(on_device, shape),
        mesh=mesh,
        in_specs=(
            P("dp", None, None, "mp"),
            P("dp", None, None, "mp"),
            P("dp", None, None, "mp"),
            P("dp"),
            P("dp", None),
            P("dp", None),
            P(),
        ),
        out_specs=P("dp", "mp"),
        check_vma=False,
    )
```

```python
import functools

import jax
import jax.numpy as jnp
from jax import lax
from jax.experimental import pallas as pl
from jax.experimental.pallas import tpu as pltpu
from jax.sharding import PartitionSpec as P

TILE = 32
CHUNK = 256


def kernel(
    sizes,
    flags_ref,
    owner_ref,
    mult_ref,
    pieces_ref,
    gate_hbm,
    lift_hbm,
    cot_hbm,
    out_ref,
    gate_in,
    lift_in,
    cot_ref,
    quarters,
    hid,
    cot_all,
    cot_t,
    part,
    arrived,
    tok_mine,
    tok_g,
    tok_sum,
    tok_all,
    tok_r,
    load_c,
    load_g,
    load_l,
    send_1,
    recv_1,
    send_2,
    recv_2,
    send_3,
    recv_3,
    send_up,
    send_dn,
    recv_h,
    send_p,
    recv_p,
    send_tg,
    recv_tg,
    send_tr,
    recv_tr,
):
    G, R, M, slots, toks, chunks, rows = sizes
    d = lax.axis_index("dp")
    m = lax.axis_index("mp")
    g = d // R
    r = d % R
    quarter = slots * toks // M

    def dev(g_to, r_to, m_to):
        return {"dp": g_to * R + r_to, "mp": m_to}

    def remote(src, dst, s, q, where):
        return pltpu.make_async_remote_copy(
            src_ref=src,
            dst_ref=dst,
            send_sem=s,
            recv_sem=q,
            device_id=where,
            device_id_type=pl.DeviceIdType.MESH,
        )

    def spread_copy(off):
        m_to = (m + off) % M
        return remote(
            cot_ref.at[pl.ds(pl.multiple_of(m_to * quarter, quarter), quarter)],
            quarters.at[m],
            send_1.at[off],
            recv_1.at[m],
            dev(g, r, m_to),
        )

    def spread_in(off):
        m_from = (m + off) % M
        return remote(
            quarters.at[m_from],
            quarters.at[m_from],
            send_1.at[off],
            recv_1.at[m_from],
            dev(g, r, m_from),
        )

    def cross_copy(off):
        g_to = (g + off) % G
        return remote(
            quarters.at[g_to], cot_all.at[m, g], send_2.at[off], recv_2.at[g], dev(g_to, r, m)
        )

    def cross_in(off):
        g_from = (g + off) % G
        return remote(
            quarters.at[g],
            cot_all.at[m, g_from],
            send_2.at[off],
            recv_2.at[g_from],
            dev(g_from, r, m),
        )

    def share_copy(off):
        return remote(
            cot_all.at[m], cot_all.at[m], send_3.at[off], recv_3.at[m], dev(g, r, (m + off) % M)
        )

    def share_in(off):
        m_from = (m + off) % M
        return remote(
            cot_all.at[m_from],
            cot_all.at[m_from],
            send_3.at[off],
            recv_3.at[m_from],
            dev(g, r, m_from),
        )

    def load(src, dst, c, sem):
        return pltpu.make_async_copy(
            src.at[:, pl.ds(c * CHUNK, CHUNK)], dst.at[c], sem.at[c]
        )

    def hop(c, origin, to, sems):
        return remote(
            hid.at[c, origin],
            hid.at[c, origin],
            sems.at[c, origin],
            recv_h.at[c, origin],
            dev(to, r, m),
        )

    up, down = (g + 1) % G, (g + G - 1) % G

    def pass_on(c, origin, has_next, to, sems):
        hop(c, origin, to, sems).wait_recv()

        @pl.when(has_next)
        def _():
            hop(c, origin, to, sems).start()

    def part_copy(c, off):
        r_to = (r + off) % R
        return remote(
            part.at[c, r_to], arrived.at[c, r], send_p.at[c, off], recv_p.at[c, r], dev(g, r_to, m)
        )

    def part_in(c, off):
        r_from = (r + off) % R
        return remote(
            part.at[c, r_from],
            arrived.at[c, r_from],
            send_p.at[c, off],
            recv_p.at[c, r_from],
            dev(g, r_from, m),
        )

    def tok_copy(off):
        return remote(
            tok_mine, tok_g.at[g], send_tg.at[off], recv_tg.at[g], dev((g + off) % G, r, m)
        )

    def tok_in(off):
        g_from = (g + off) % G
        return remote(
            tok_mine, tok_g.at[g_from], send_tg.at[off], recv_tg.at[g_from], dev(g_from, r, m)
        )

    def sum_copy(off):
        return remote(
            tok_sum, tok_r.at[r], send_tr.at[off], recv_tr.at[r], dev(g, (r + off) % R, m)
        )

    def sum_in(off):
        r_from = (r + off) % R
        return remote(
            tok_sum, tok_r.at[r_from], send_tr.at[off], recv_tr.at[r_from], dev(g, r_from, m)
        )

    def over_r(body):
        def step(off, carry):
            body(off)
            return carry

        lax.fori_loop(1, R, step, 0)

    load_cot = pltpu.make_async_copy(cot_hbm, cot_ref, load_c)
    load_cot.start()
    for c in range(chunks):
        load(gate_hbm, gate_in, c, load_g).start()
        load(lift_hbm, lift_in, c, load_l).start()

    barrier = pltpu.get_barrier_semaphore()

    def greet(where):
        pl.semaphore_signal(
            barrier, inc=1, device_id=where, device_id_type=pl.DeviceIdType.MESH
        )

    for off in range(1, M):
        greet(dev(g, r, (m + off) % M))
    for off in range(1, G):
        greet(dev((g + off) % G, r, m))
    over_r(lambda off: greet(dev(g, (r + off) % R, m)))
    load_cot.wait()
    quarters[m] = cot_ref[pl.ds(pl.multiple_of(m * quarter, quarter), quarter), :]
    pl.semaphore_wait(barrier, M - 1 + G - 1 + R - 1)

    for off in range(1, M):
        spread_copy(off).start()

    flag = flags_ref[0].astype(jnp.float32)
    scales = []
    token_sum = jnp.float32(0)
    row = lax.broadcasted_iota(jnp.int32, (toks, CHUNK), 0)
    for k in range(slots):
        live = pieces_ref[owner_ref[0, k]] * TILE
        weight = flag * mult_ref[0, k].astype(jnp.float32)
        scales.append(jnp.where(row < live, weight, 0.0))
        token_sum = token_sum + weight * live.astype(jnp.float32)

    for c in range(chunks):
        load(gate_hbm, gate_in, c, load_g).wait()
        load(lift_hbm, lift_in, c, load_l).wait()
        for k in range(slots):
            rk = pl.ds(k * toks, toks)
            v = gate_in[c, rk, :].astype(jnp.float32)
            u = lift_in[c, rk, :].astype(jnp.float32)
            h = v / (1.0 + jnp.exp(-v)) * u * scales[k]
            hid[c, g, rk, :] = h.astype(jnp.bfloat16)
        if c == 0:
            tok_mine[...] = jnp.full(tok_mine.shape, token_sum, jnp.float32)

        @pl.when(g < G - 1)
        def _():
            hop(c, g, up, send_up).start()

        @pl.when(g > 0)
        def _():
            hop(c, g, down, send_dn).start()

        if c == 0:
            for off in range(1, G):
                tok_copy(off).start()
            for off in range(1, M):
                spread_in(off).wait_recv()
            cot_all[m, g] = quarters[g]
            for off in range(1, G):
                cross_copy(off).start()

    for off in range(1, G):
        cross_in(off).wait_recv()
    for off in range(1, M):
        share_copy(off).start()
    for off in range(1, M):
        share_in(off).wait_recv()

    for i in range(G):
        n = slots * toks
        block = jnp.concatenate([cot_all[j, i] for j in range(M)], axis=0)
        cot_t[:, pl.ds(i * n, n)] = block.T

    def add_tokens(off, total):
        sum_in(off).wait_recv()
        return total + tok_r[(r + off) % R]

    def finish(c):
        if c == 0:
            tok_all[...] = lax.fori_loop(1, R, add_tokens, tok_sum[...])
        inverse = 1.0 / tok_all[0:1, 0:1]
        cols = pl.ds(c * CHUNK, CHUNK)

        def add_part(off):
            part_in(c, off).wait_recv()
            out_ref[:, cols] = out_ref[:, cols] + arrived[c, (r + off) % R].astype(jnp.float32)

        over_r(add_part)
        out_ref[:, cols] = out_ref[:, cols] * inverse

    for c in range(chunks):
        for k in range(1, G):

            @pl.when(g >= k)
            def _():
                pass_on(c, (g + G - k) % G, g < G - 1, up, send_up)

            @pl.when(g + k < G)
            def _():
                pass_on(c, (g + k) % G, g > 0, down, send_dn)

        block = hid[c].reshape(G * slots * toks, CHUNK)
        if c == 0:
            total = tok_mine[...]
            for off in range(1, G):
                tok_in(off).wait_recv()
                total = total + tok_g[(g + off) % G]
            tok_sum[...] = total

        def other(off):
            r_to = (r + off) % R
            left = cot_t[pl.ds(pl.multiple_of(r_to * rows, rows), rows), :]
            prod = jnp.dot(left, block, preferred_element_type=jnp.float32)
            part[c, r_to] = prod.astype(jnp.bfloat16)
            part_copy(c, off).start()

        over_r(other)
        if c == 0:
            over_r(lambda off: sum_copy(off).start())
        left = cot_t[pl.ds(pl.multiple_of(r * rows, rows), rows), :]
        out_ref[:, pl.ds(c * CHUNK, CHUNK)] = jnp.dot(
            left, block, preferred_element_type=jnp.float32
        )
        if c >= 2:
            finish(c - 2)

    for c in range(max(chunks - 2, 0), chunks):
        finish(c)

    for off in range(1, M):
        spread_copy(off).wait_send()
        share_copy(off).wait_send()

    for off in range(1, G):
        tok_copy(off).wait_send()
        cross_copy(off).wait_send()

    for c in range(chunks):
        for i in range(G):

            @pl.when(jnp.logical_and(i <= g, g < G - 1))
            def _():
                hop(c, i, up, send_up).wait_send()

            @pl.when(jnp.logical_and(i >= g, g > 0))
            def _():
                hop(c, i, down, send_dn).wait_send()

    def drain(off):
        sum_copy(off).wait_send()
        for c in range(chunks):
            part_copy(c, off).wait_send()

    over_r(drain)


def on_device(
    mesh_shape,
    gating_logits,
    lifted_hidden_values,
    loss_output_grad,
    arrival_flags,
    block_owner_map,
    decoder_multipliers,
    block_piece_number,
):
    dp, M = mesh_shape
    G = M
    R = dp // G
    _, slots, toks, width = gating_logits.shape
    feats = loss_output_grad.shape[3]
    rows = feats * M // dp
    chunks = width // CHUNK
    n = slots * toks
    sizes = (G, R, M, slots, toks, chunks, rows)
    smem = pl.BlockSpec(memory_space=pltpu.SMEM)
    vmem = pl.BlockSpec(memory_space=pltpu.VMEM)
    dma = pltpu.SemaphoreType.DMA
    bf, f32 = jnp.bfloat16, jnp.float32
    return pl.pallas_call(
        functools.partial(kernel, sizes),
        out_shape=jax.ShapeDtypeStruct((rows, width), f32),
        in_specs=[smem] * 4 + [pl.BlockSpec(memory_space=pl.ANY)] * 3,
        out_specs=vmem,
        scratch_shapes=[
            pltpu.VMEM((chunks, n, CHUNK), bf),
            pltpu.VMEM((chunks, n, CHUNK), bf),
            pltpu.VMEM((n, feats), bf),
            pltpu.VMEM((M, n // M, feats), bf),
            pltpu.VMEM((chunks, G, n, CHUNK), bf),
            pltpu.VMEM((M, G, n // M, feats), bf),
            pltpu.VMEM((feats, G * n), bf),
            pltpu.VMEM((chunks, R, rows, CHUNK), bf),
            pltpu.VMEM((chunks, R, rows, CHUNK), bf),
            pltpu.VMEM((8, 128), f32),
            pltpu.VMEM((G, 8, 128), f32),
            pltpu.VMEM((8, 128), f32),
            pltpu.VMEM((8, 128), f32),
            pltpu.VMEM((R, 8, 128), f32),
            dma,
            dma((chunks,)),
            dma((chunks,)),
            dma((M,)),
            dma((M,)),
            dma((G,)),
            dma((G,)),
            dma((M,)),
            dma((M,)),
            dma((chunks, G)),
            dma((chunks, G)),
            dma((chunks, G)),
            dma((chunks, R)),
            dma((chunks, R)),
            dma((G,)),
            dma((G,)),
            dma((R,)),
            dma((R,)),
        ],
        compiler_params=pltpu.CompilerParams(
            collective_id=0, has_side_effects=True
        ),
    )(
        arrival_flags,
        block_owner_map,
        decoder_multipliers,
        block_piece_number,
        gating_logits.reshape(n, width),
        lifted_hidden_values.reshape(n, width),
        loss_output_grad.reshape(n, feats),
    )


def solution(mesh):
    shape = (mesh.shape["dp"], mesh.shape["mp"])
    return jax.shard_map(
        functools.partial(on_device, shape),
        mesh=mesh,
        in_specs=(
            P("dp", None, None, "mp"),
            P("dp", None, None, "mp"),
            P("dp", None, None, "mp"),
            P("dp"),
            P("dp", None),
            P("dp", None),
            P(),
        ),
        out_specs=P("dp", "mp"),
        check_vma=False,
    )
```
